32 devices in a mesh: files: 8 (over z, y), rep: 4 (over x, core).
Axes of the slice: x: 2, y: 2, z: 4, core: 2. Of those that a mesh axis runs over, the one named last changes fastest.
Arguments:
- tile_id: int32 [131072], P(('files', 'rep')), may hold values from 0 to 127, as said below
- pix_row: int32 [131072], P(('files', 'rep')), may hold values from 0 to 31
- pix_col: int32 [131072], P(('files', 'rep')), may hold values from 0 to 127
- point_value: bfloat16 [131072], P(('files', 'rep')), may hold values from -6 to 6
Outputs:
- tile_sums: float32 [128, 32, 128], P('files', 'rep')
The draws below stay inside these ranges and needn't reach their ends.
Inputs may be any that keep to these rules, and one draw needn't show every extreme that they name: `tile_id`: of the points of one device, at most 2048 lie in tiles of one file group (tile id modulo 8), and on every device some group holds exactly 2048 of them.
All inputs are finite; a program needn't handle non-finite values.
Results may differ from the reference program's by a relative error of at most 0.0003.
Values sent between devices are 32-bit elements; how exact they have to be, the bound alone decides.
A program may use at most 64 MiB of HBM per device.

```python
import jax
import jax.numpy as jnp

TC = 128
TR = 32
PTS_DEV = 4096
TILES = 128
TILE_OWN = 16
CAP = 2048
POINTS = 131072
N_FILES = 8
N_REP = 4


def draw_tile_id(key, part):
    device_count = POINTS // PTS_DEV
    tier_most = N_FILES // 8
    middle_low = max(1, CAP // 4)
    middle_high = max(middle_low, CAP // 2)

    def one_device(device_key):
        key_order = jax.random.fold_in(device_key, 1)
        key_local = jax.random.fold_in(device_key, 2)
        key_mixing = jax.random.fold_in(device_key, 3)
        key_heavy = jax.random.fold_in(device_key, 4)
        key_middle = jax.random.fold_in(device_key, 5)
        key_size = jax.random.fold_in(device_key, 6)
        owner_order = jax.random.permutation(key_order, N_FILES)
        heavy_count = jax.random.randint(key_heavy, (), 1, tier_most + 1)
        middle_count = jax.random.randint(key_middle, (), 0, tier_most + 1)
        middle_size = jax.random.randint(key_size, (), middle_low, middle_high + 1)
        slot_index = jnp.arange(PTS_DEV, dtype=jnp.int32)
        heavy_end = heavy_count * CAP
        middle_end = heavy_end + middle_count * middle_size
        rest_owners = N_FILES - heavy_count - middle_count
        rank_heavy = slot_index // CAP
        rank_middle = heavy_count + (slot_index - heavy_end) // middle_size
        rank_rest = heavy_count + middle_count + (slot_index - middle_end) % rest_owners
        pick_rank = jnp.where(slot_index < heavy_end, rank_heavy, jnp.where(slot_index < middle_end, rank_middle, rank_rest))
        pick_rank = jnp.clip(pick_rank, 0, N_FILES - 1).astype(jnp.int32)
        tile_owner = owner_order[pick_rank]
        tile_local = jax.random.randint(key_local, (PTS_DEV,), 0, TILE_OWN)
        tile_ids = tile_owner + N_FILES * tile_local
        return jax.random.permutation(key_mixing, tile_ids)
    device_keys = jax.random.split(jax.random.fold_in(key, 11), device_count)
    return jax.vmap(one_device)(device_keys).reshape(POINTS).astype(jnp.int32)


def draw_pix_row(key, part):
    device_count = POINTS // PTS_DEV
    quarter = TR // N_REP

    def one_device(device_key):
        hot_quarter = jax.random.randint(jax.random.fold_in(device_key, 1), (), 0, N_REP)
        hot_share = jax.random.randint(jax.random.fold_in(device_key, 2), (), 3, 8)
        pick_tenth = jax.random.randint(jax.random.fold_in(device_key, 3), (PTS_DEV,), 0, 10)
        inner_row = jax.random.randint(jax.random.fold_in(device_key, 4), (PTS_DEV,), 0, quarter)
        spread_row = jax.random.randint(jax.random.fold_in(device_key, 5), (PTS_DEV,), 0, TR)
        return jnp.where(pick_tenth < hot_share, hot_quarter * quarter + inner_row, spread_row)
    device_keys = jax.random.split(jax.random.fold_in(key, 21), device_count)
    return jax.vmap(one_device)(device_keys).reshape(POINTS).astype(jnp.int32)


def with_ends(values, stream_key, smallest, top_value):
    extent = values.shape
    index_at = [jax.random.randint(jax.random.fold_in(stream_key, axis), (), 0, extent[axis]) for axis in range(len(extent))]
    values = values.at[tuple(index_at)].set(smallest)
    longest = extent.index(max(extent))
    index_at[longest] = (index_at[longest] + 1) % extent[longest]
    return values.at[tuple(index_at)].set(top_value)


def levels(own_key, shape, shards, least, largest):
    loudness = 1.0
    for dim, blocks in shards:
        draws = jax.random.uniform(jax.random.fold_in(jax.random.fold_in(own_key, 6), dim), (blocks,), jnp.float32, least / len(shards), largest / len(shards))
        loudness = loudness * jnp.repeat(jnp.exp(draws), shape[dim] // blocks).reshape((-1,) + (1,) * (len(shape) - 1 - dim))
    return loudness


def centred(key, shape, scale, limit, shards=(), kind=jnp.bfloat16):
    result = jax.random.normal(key, shape, jnp.float32) * scale
    if len(shards) > 0:
        result = levels(key, shape, shards, -0.22, 0.18) * result
    return jnp.clip(result, min=-limit, max=limit).astype(kind)


def setup_inputs(seed: int = 0) -> dict:
    keys = jax.random.split(jax.random.key(seed), 5)
    return {
        "tile_id": draw_tile_id(jax.random.fold_in(keys[4], 71), 0),
        "pix_row": draw_pix_row(jax.random.fold_in(keys[4], 71), 0),
        "pix_col": with_ends(jax.random.randint(keys[2], (POINTS,), 0, TC), jax.random.fold_in(keys[2], 1), 0, TC - 1).astype(jnp.int32),
        "point_value": centred(keys[3], (POINTS,), 1.0, 6.0, ((0, 32),)),
    }


def reference(tile_id, pix_row, pix_col, point_value):
    tile_owner = tile_id % N_FILES
    tile_local = tile_id // N_FILES
    owned_slot = tile_owner * TILE_OWN + tile_local
    flat_cell = (owned_slot * TR + pix_row) * TC + pix_col
    summed = jax.ops.segment_sum(point_value.astype(jnp.float32), flat_cell.astype(jnp.int32), num_segments=TILES * TR * TC)
    return summed.reshape(TILES, TR, TC)
```

```python
import functools

import jax
import jax.numpy as jnp
from jax import lax
from jax.experimental import pallas as pl
from jax.experimental.pallas import tpu as pltpu
from jax.sharding import PartitionSpec as P

LANES = 128
WIDE = 256
TR = 32
TILES = 128
MESH = pl.DeviceIdType.MESH


def flipped(index, mask, count):
    out = index
    bit = 1
    while bit < count:
        if mask & bit:
            out = out + (1 - 2 * ((index // bit) % 2)) * bit
        bit *= 2
    return out


def kernel(nf, nr, owned, quarter, tile_ref, row_ref, col_ref, val_ref, out_ref,
           pack, got, acc, parts, gsend, grecv, rsend, rrecv):
    f = lax.axis_index("files")
    r = lax.axis_index("rep")
    half = owned * quarter // 2
    band = nr * half
    blocks = tile_ref.shape[0]

    barrier = pltpu.get_barrier_semaphore()
    for k in range(1, nf):
        pl.semaphore_signal(barrier, inc=1, device_id={"files": flipped(f, k, nf)}, device_id_type=MESH)
    for k in range(1, nr):
        pl.semaphore_signal(barrier, inc=1, device_id={"rep": flipped(r, k, nr)}, device_id_type=MESH)

    tile = tile_ref[...]
    prow = row_ref[...]
    owner = tile % nf
    inner = (tile // nf) * quarter + prow % quarter
    cell = (owner * band + (prow // quarter) * half + inner % half) * WIDE
    cell = cell + (inner // half) * LANES + col_ref[...]
    pack[0:blocks, :] = cell.astype(jnp.float32)
    pack[blocks:, :] = val_ref[...]
    acc[...] = jnp.zeros_like(acc)

    pl.semaphore_wait(barrier, nf + nr - 2)

    sends = []
    for k in range(1, nf):
        copy = pltpu.make_async_remote_copy(
            src_ref=pack, dst_ref=got.at[k], send_sem=gsend.at[k], recv_sem=grecv.at[k],
            device_id={"files": flipped(f, k, nf)}, device_id_type=MESH)
        copy.start()
        sends.append(copy)

    def add_points(cells, values):
        first = f * band
        row = jnp.floor(cells * (1.0 / WIDE))
        col = cells - row * WIDE
        row = row - first.astype(jnp.float32)
        col_t = jnp.transpose(col)
        ids16 = lax.broadcasted_iota(jnp.int32, (16, LANES), 0)
        lane = lax.broadcasted_iota(jnp.int32, (LANES, LANES), 1)
        lane_lo = lane.astype(jnp.float32).astype(jnp.bfloat16)
        lane_hi = (lane + LANES).astype(jnp.float32).astype(jnp.bfloat16)
        one = jnp.ones((), jnp.bfloat16)
        zero = jnp.zeros((), jnp.bfloat16)
        lhs = []
        rhs = []
        for j in range(blocks):
            row16 = jnp.broadcast_to(row[j:j + 1, :], (16, LANES)).astype(jnp.bfloat16)
            val16 = jnp.broadcast_to(values[j:j + 1, :], (16, LANES)).astype(jnp.bfloat16)
            lhs.append(jnp.concatenate([
                jnp.where(row16 == (ids16 + 16 * i).astype(jnp.float32).astype(jnp.bfloat16), val16, zero)
                for i in range(band // 16)], axis=0))
            colb = jnp.broadcast_to(col_t[:, j:j + 1], (LANES, LANES)).astype(jnp.bfloat16)
            rhs.append(jnp.concatenate([
                jnp.where(colb == lane_lo, one, zero),
                jnp.where(colb == lane_hi, one, zero)], axis=1))
        total = jnp.dot(jnp.concatenate(lhs, axis=1), jnp.concatenate(rhs, axis=0),
                        preferred_element_type=jnp.float32)
        for q in range(nr):
            acc[q] += total[q * half:(q + 1) * half, :]

    add_points(pack[0:blocks, :], pack[blocks:, :])

    def step(k, carry):
        pltpu.make_async_remote_copy(
            src_ref=pack, dst_ref=got.at[k], send_sem=gsend.at[k], recv_sem=grecv.at[k],
            device_id={"files": (f + 1) % nf}, device_id_type=MESH).wait_recv()
        add_points(got[k, 0:blocks, :], got[k, blocks:, :])
        return carry

    lax.fori_loop(1, nf, step, 0)

    backs = []
    for k in range(1, nr):
        peer = flipped(r, k, nr)
        copy = pltpu.make_async_remote_copy(
            src_ref=acc.at[peer], dst_ref=parts.at[k], send_sem=rsend.at[k], recv_sem=rrecv.at[k],
            device_id={"rep": peer}, device_id_type=MESH)
        copy.start()
        backs.append(copy)
    total = acc[r]
    for k in range(1, nr):
        backs[k - 1].wait_recv()
        total = total + parts[k]
    out_ref[0:half, :] = total[:, :LANES]
    out_ref[half:, :] = total[:, LANES:]
    for copy in sends + backs:
        copy.wait_send()


def solution(mesh):
    nf = mesh.shape["files"]
    nr = mesh.shape["rep"]
    owned = TILES // nf
    quarter = TR // nr
    half = owned * quarter // 2

    def per_device(tile_id, pix_row, pix_col, point_value):
        blocks = tile_id.shape[0] // LANES
        shape = (blocks, LANES)
        vmem = pl.BlockSpec(memory_space=pltpu.VMEM)
        out = pl.pallas_call(
            functools.partial(kernel, nf, nr, owned, quarter),
            out_shape=jax.ShapeDtypeStruct((owned * quarter, LANES), jnp.float32),
            in_specs=[vmem] * 4,
            out_specs=vmem,
            scratch_shapes=[
                pltpu.VMEM((2 * blocks, LANES), jnp.float32),
                pltpu.VMEM((nf, 2 * blocks, LANES), jnp.float32),
                pltpu.VMEM((nr, half, WIDE), jnp.float32),
                pltpu.VMEM((nr, half, WIDE), jnp.float32),
                pltpu.SemaphoreType.DMA((nf,)),
                pltpu.SemaphoreType.DMA((nf,)),
                pltpu.SemaphoreType.DMA((nr,)),
                pltpu.SemaphoreType.DMA((nr,)),
            ],
            compiler_params=pltpu.CompilerParams(collective_id=0, has_side_effects=True),
        )(tile_id.reshape(shape), pix_row.reshape(shape), pix_col.reshape(shape),
          point_value.astype(jnp.float32).reshape(shape))
        return out.reshape(owned, quarter, LANES)

    both = P(("files", "rep"))
    return jax.shard_map(per_device, mesh=mesh, in_specs=(both,) * 4,
                         out_specs=P("files", "rep", None), check_vma=False)
```

```python
import functools

import jax
import jax.numpy as jnp
from jax import lax
from jax.experimental import pallas as pl
from jax.experimental.pallas import tpu as pltpu
from jax.sharding import PartitionSpec as P

LANES = 128
WIDE = 256
TR = 32
TILES = 128
SPLIT = 1
ORDER = (1, 2, 6, 3, 7, 4, 5)
MESH = pl.DeviceIdType.MESH


def flipped(index, mask, count):
    out = index
    bit = 1
    while bit < count:
        if mask & bit:
            out = out + (1 - 2 * ((index // bit) % 2)) * bit
        bit *= 2
    return out


def kernel(nf, nr, owned, quarter, tile_ref, row_ref, col_ref, val_ref, out_ref,
           tile_in, row_in, col_in, val_in, got, acc, parts,
           isem, gsend, grecv, rsend, rrecv):
    f = lax.axis_index("files")
    r = lax.axis_index("rep")
    half = owned * quarter // 2
    band = nr * half
    blocks = tile_ref.shape[0]

    loads = []
    for i, (src, dst) in enumerate(((tile_ref, tile_in), (row_ref, row_in), (col_ref, col_in), (val_ref, val_in))):
        load = pltpu.make_async_copy(src, dst, isem.at[i])
        load.start()
        loads.append(load)
    barrier = pltpu.get_barrier_semaphore()
    for k in range(1, nf):
        pl.semaphore_signal(barrier, inc=1, device_id={"files": flipped(f, k, nf)}, device_id_type=MESH)
    for k in range(1, nr):
        pl.semaphore_signal(barrier, inc=1, device_id={"rep": flipped(r, k, nr)}, device_id_type=MESH)

    for load in loads:
        load.wait()
    tile = tile_in[...]
    prow = row_in[...]
    owner = tile % nf
    inner = (tile // nf) * quarter + prow % quarter
    cell = (owner * band + (prow // quarter) * half + inner % half) * WIDE
    cell = cell + (inner // half) * LANES + col_in[...]
    got[0, 0:blocks, :] = cell.astype(jnp.float32)
    got[0, blocks:, :] = val_in[...].astype(jnp.float32)

    pl.semaphore_wait(barrier, nf + nr - 2)

    sends = []
    for i, k in enumerate(ORDER if nf == 8 else range(1, nf), 1):
        copy = pltpu.make_async_remote_copy(
            src_ref=got.at[0], dst_ref=got.at[i], send_sem=gsend.at[i], recv_sem=grecv.at[i],
            device_id={"files": flipped(f, k, nf)}, device_id_type=MESH)
        copy.start()
        sends.append(copy)

    ids16 = lax.broadcasted_iota(jnp.int32, (16, LANES), 0)
    lane = lax.broadcasted_iota(jnp.int32, (LANES, LANES), 1)
    lane_lo = lane.astype(jnp.float32).astype(jnp.bfloat16)
    lane_hi = (lane + LANES).astype(jnp.float32).astype(jnp.bfloat16)
    one = jnp.ones((), jnp.bfloat16)
    zero = jnp.zeros((), jnp.bfloat16)
    first = (f * band).astype(jnp.float32)

    span = blocks // SPLIT

    def add_points(cells, values):
        row = jnp.floor(cells * (1.0 / WIDE))
        col_t = jnp.transpose(cells - row * WIDE)
        row = row - first
        lhs = []
        rhs = []
        for j in range(span):
            row16 = jnp.broadcast_to(row[j:j + 1, :], (16, LANES)).astype(jnp.bfloat16)
            val16 = jnp.broadcast_to(values[j:j + 1, :], (16, LANES)).astype(jnp.bfloat16)
            lhs.append(jnp.concatenate([
                jnp.where(row16 == (ids16 + 16 * i).astype(jnp.float32).astype(jnp.bfloat16), val16, zero)
                for i in range(band // 16)], axis=0))
            colb = jnp.broadcast_to(col_t[:, j:j + 1], (LANES, LANES)).astype(jnp.bfloat16)
            rhs.append(jnp.concatenate([
                jnp.where(colb == lane_lo, one, zero),
                jnp.where(colb == lane_hi, one, zero)], axis=1))
        total = jnp.dot(jnp.concatenate(lhs, axis=1), jnp.concatenate(rhs, axis=0),
                        preferred_element_type=jnp.float32)
        for q in range(nr):
            acc[q] += total[q * half:(q + 1) * half, :]

    acc[...] = jnp.zeros_like(acc)

    def step(t, carry):
        i = t // SPLIT
        at = (t % SPLIT) * span

        @pl.when(jnp.logical_and(i > 0, t % SPLIT == 0))
        def _():
            pltpu.make_async_remote_copy(
                src_ref=got.at[0], dst_ref=got.at[i], send_sem=gsend.at[i], recv_sem=grecv.at[i],
                device_id={"files": (f + 1) % nf}, device_id_type=MESH).wait_recv()

        add_points(got[i, pl.ds(pl.multiple_of(at, 8), span), :],
                   got[i, pl.ds(pl.multiple_of(blocks + at, 8), span), :])
        return carry

    lax.fori_loop(0, nf * SPLIT, step, 0)

    backs = []
    for k in range(1, nr):
        peer = flipped(r, k, nr)
        copy = pltpu.make_async_remote_copy(
            src_ref=acc.at[peer], dst_ref=parts.at[k], send_sem=rsend.at[k], recv_sem=rrecv.at[k],
            device_id={"rep": peer}, device_id_type=MESH)
        copy.start()
        backs.append(copy)
    total = acc[r]
    for k in range(1, nr):
        backs[k - 1].wait_recv()
        total = total + parts[k]
    out_ref[0:half, :] = total[:, :LANES]
    out_ref[half:, :] = total[:, LANES:]
    for copy in sends + backs:
        copy.wait_send()


def solution(mesh):
    nf = mesh.shape["files"]
    nr = mesh.shape["rep"]
    owned = TILES // nf
    quarter = TR // nr
    half = owned * quarter // 2

    def per_device(tile_id, pix_row, pix_col, point_value):
        blocks = tile_id.shape[0] // LANES
        shape = (blocks, LANES)
        vmem = pl.BlockSpec(memory_space=pltpu.VMEM)
        out = pl.pallas_call(
            functools.partial(kernel, nf, nr, owned, quarter),
            out_shape=jax.ShapeDtypeStruct((owned * quarter, LANES), jnp.float32),
            in_specs=[pl.BlockSpec(memory_space=pl.ANY)] * 4,
            out_specs=vmem,
            scratch_shapes=[
                pltpu.VMEM(shape, jnp.int32),
                pltpu.VMEM(shape, jnp.int32),
                pltpu.VMEM(shape, jnp.int32),
                pltpu.VMEM(shape, point_value.dtype),
                pltpu.VMEM((nf, 2 * blocks, LANES), jnp.float32),
                pltpu.VMEM((nr, half, WIDE), jnp.float32),
                pltpu.VMEM((nr, half, WIDE), jnp.float32),
                pltpu.SemaphoreType.DMA((4,)),
                pltpu.SemaphoreType.DMA((nf,)),
                pltpu.SemaphoreType.DMA((nf,)),
                pltpu.SemaphoreType.DMA((nr,)),
                pltpu.SemaphoreType.DMA((nr,)),
            ],
            compiler_params=pltpu.CompilerParams(collective_id=0, has_side_effects=True),
        )(tile_id.reshape(shape), pix_row.reshape(shape), pix_col.reshape(shape),
          point_value.reshape(shape))
        return out.reshape(owned, quarter, LANES)

    both = P(("files", "rep"))
    return jax.shard_map(per_device, mesh=mesh, in_specs=(both,) * 4,
                         out_specs=P("files", "rep", None), check_vma=False)
```
